32 devices in a mesh: batch: 8 (over z, x), seq: 4 (over y, core).
Axes of the slice: x: 2, y: 2, z: 4, core: 2. Of those that a mesh axis runs over, the one named last changes fastest.
Arguments:
- hidden_in: bfloat16 [8, 512, 2048], P('batch', 'seq'), may hold values from -6 to 6
- queries: bfloat16 [8, 512, 2048], P('batch', 'seq'), may hold values from -5 to 5
- key_states: bfloat16 [8, 512, 512], P('batch', 'seq'), may hold values from -12 to 12
- value_states: bfloat16 [8, 512, 512], P('batch', 'seq'), may hold values from -6 to 6
- grad_out: bfloat16 [8, 512, 2048], P('batch', 'seq'), may hold values from -6 to 6
- log_sums: float32 [8, 16, 512], P('batch', None, 'seq'), may hold values from -700 to 700, as said below
- deltas: float32 [8, 16, 512], P('batch', None, 'seq'), may hold values from -6 to 6
- block_order: int32 [8], replicated, may hold values from 0 to 7, as said below
Outputs:
- grad_queries: bfloat16 [8, 512, 2048], P('batch', 'seq')
- grad_keys: bfloat16 [8, 512, 512], P('batch', 'seq')
- grad_values: bfloat16 [8, 512, 512], P('batch', 'seq')
- key_wgrad: float32 [2048, 512], P(('batch', 'seq'))
- value_wgrad: float32 [2048, 512], P(('batch', 'seq'))
The draws below stay inside these ranges and needn't reach their ends.
Inputs may be any that keep to these rules, and one draw needn't show every extreme that they name: `block_order`: entries 2i and 2i+1 name blocks c and 7 - c for some c, in either order; the 8 entries together are a permutation of 0 to 7. `log_sums`: each entry lies within 0.1 of the log of the sum over visible j of exp(scores[b,h,i,j]).
All inputs are finite; a program needn't handle non-finite values.
Results may differ from the reference program's by a relative error of at most 0.0049.
Values may be sent and summed in bfloat16 or wider, within the bound.
A program may use at most 64 MiB of HBM per device.

```python
import math
import jax
import jax.numpy as jnp
from jax import lax

HQ = 16
HK = 4
DH = 128
DIN = 2048
SEQ = 512
BATCH = 8
BLOCK = 64
BLOCKS = 8
GROUP = 4
QW = 2048
KW = 512


def draw_queries(key, part):
    normal_part = jnp.clip(jax.random.normal(jax.random.fold_in(key, 11), (BATCH, SEQ, HQ * DH), jnp.float32), -4.0, 4.0)
    return normal_part.astype(jnp.bfloat16)


def draw_key_states(key, part):
    normal_part = jnp.clip(jax.random.normal(jax.random.fold_in(key, 13), (BATCH, SEQ, HK * DH), jnp.float32), -4.0, 4.0)
    return normal_part.astype(jnp.bfloat16)


def draw_block_order(key, part):
    pair_key, flip_key = jax.random.split(jax.random.fold_in(key, 29))
    pair_ids = jax.random.permutation(pair_key, BLOCKS // 2).astype(jnp.int32)
    flip_bits = jax.random.randint(flip_key, (BLOCKS // 2,), 0, 2)
    first_block = jnp.where(flip_bits == 1, BLOCKS - 1 - pair_ids, pair_ids)
    second_block = BLOCKS - 1 - first_block
    return jnp.stack([first_block, second_block], axis=1).reshape(BLOCKS).astype(jnp.int32)


def draw_log_sums(key, part):
    query_all = draw_queries(key, part).astype(jnp.float32)
    key_all = draw_key_states(key, part).astype(jnp.float32)
    order = draw_block_order(key, part)
    row_ids = jnp.arange(SEQ, dtype=jnp.int32)
    position = order[row_ids // BLOCK] * BLOCK + row_ids % BLOCK
    visible = position[None, :] <= position[:, None]

    def one_group(group_ops):
        group_queries, group_keys = group_ops
        scores = jnp.einsum('igd,jd->gij', group_queries, group_keys) * (1.0 / math.sqrt(DH))
        scores = jnp.where(visible[None, :, :], scores, -jnp.inf)
        return jax.nn.logsumexp(scores, axis=-1)

    def one_sequence(seq_ops):
        seq_queries, seq_keys = seq_ops
        queries_head = jnp.moveaxis(seq_queries.reshape(SEQ, HK, GROUP, DH), 1, 0)
        keys_head = jnp.moveaxis(seq_keys.reshape(SEQ, HK, DH), 1, 0)
        return lax.map(one_group, (queries_head, keys_head)).reshape(HQ, SEQ)
    exact = lax.map(one_sequence, (query_all, key_all))
    noise = jax.random.uniform(jax.random.fold_in(key, 41), (BATCH, HQ, SEQ), jnp.float32, -0.1, 0.1)
    return (exact + noise).astype(jnp.float32)


def spiked(result, stream_key, source, target, blocks, factor):
    def block_of(dim):
        return (jnp.arange(result.shape[dim]) // (result.shape[dim] // blocks)).reshape((-1,) + (1,) * (result.ndim - 1 - dim))

    one_side = jax.random.permutation(stream_key, blocks)[block_of(target)]
    far = (block_of(target) + blocks // 2) % blocks
    return jnp.where((block_of(source) == one_side) | (block_of(source) == far), factor * result, result)


def block_scale(rng, shape, cuts, smallest, top_value):
    def one(dim, blocks):
        steps = jax.random.uniform(jax.random.fold_in(jax.random.fold_in(rng, 6), dim), (blocks,), jnp.float32, smallest / len(cuts), top_value / len(cuts))
        return jnp.repeat(jnp.exp(steps), shape[dim] // blocks).reshape((-1,) + (1,) * (len(shape) - dim - 1))

    factor_of = one(*cuts[0])
    for cut in cuts[1:]:
        factor_of = factor_of * one(*cut)
    return factor_of


def scatter_about(rng, dims, width, reach, cuts=(), kind=jnp.bfloat16):
    loudness = block_scale(rng, dims, cuts, -0.22, 0.18) if cuts else 1.0
    entries = jax.random.normal(rng, dims, jnp.float32) * width * loudness
    return jnp.minimum(jnp.maximum(entries, -reach), reach).astype(kind)


def heavy_noise(rng, dims, width, reach, cuts, heavy, held_as=jnp.bfloat16):
    result = width * jax.random.normal(rng, dims, jnp.float32)
    if cuts:
        result = result * block_scale(rng, dims, cuts, -0.22, 0.18)
    return jnp.clip(spiked(result, jax.random.fold_in(rng, 3), *heavy), -reach, reach).astype(held_as)


def setup_inputs(seed: int = 0) -> dict:
    arg_keys = jax.random.split(jax.random.key(seed), 9)
    hidden_in = heavy_noise(arg_keys[0], (BATCH, SEQ, DIN), 1.0, 6.0, ((0, 8), (1, 4)), (1, 2, 4, 2.0))
    queries = draw_queries(jax.random.fold_in(arg_keys[8], 71), 0)
    key_states = draw_key_states(jax.random.fold_in(arg_keys[8], 71), 0)
    value_states = scatter_about(arg_keys[3], (BATCH, SEQ, KW), 1.0, 6.0, ((0, 8), (1, 4)))
    grad_out = scatter_about(arg_keys[4], (BATCH, SEQ, QW), 1.0, 6.0, ((0, 8), (1, 4)))
    log_sums = draw_log_sums(jax.random.fold_in(arg_keys[8], 71), 0)
    deltas = scatter_about(arg_keys[6], (BATCH, HQ, SEQ), 1.0, 6.0, ((0, 8), (2, 4)), jnp.float32)
    block_order = draw_block_order(jax.random.fold_in(arg_keys[8], 71), 0)
    return {"hidden_in": hidden_in, "queries": queries, "key_states": key_states, "value_states": value_states, "grad_out": grad_out, "log_sums": log_sums, "deltas": deltas, "block_order": block_order}


def group_grads(operands, position):
    group_queries, group_keys, group_values, group_cots, group_lse, group_deltas = operands
    scale_factor = 1.0 / math.sqrt(DH)
    query_full = group_queries.astype(jnp.float32)
    key_full = group_keys.astype(jnp.float32)
    value_full = group_values.astype(jnp.float32)
    grad_full = group_cots.astype(jnp.float32)
    scores = jnp.einsum('igd,jd->gij', query_full, key_full) * scale_factor
    visible = position[None, :] <= position[:, None]
    scores = jnp.where(visible[None, :, :], scores, -jnp.inf)
    probs = jnp.exp(scores - group_lse[..., None])
    grad_probs = jnp.einsum('igd,jd->gij', grad_full, value_full)
    grad_scores = (probs * (grad_probs - group_deltas[..., None]) * scale_factor).astype(jnp.bfloat16)
    grad_scores = lax.optimization_barrier(grad_scores).astype(jnp.float32)
    probs_low = lax.optimization_barrier(probs.astype(jnp.bfloat16)).astype(jnp.float32)
    query_grad = jnp.einsum('gij,jd->igd', grad_scores, key_full)
    key_grad = jnp.einsum('gij,igd->jd', grad_scores, query_full)
    value_grad = jnp.einsum('gij,igd->jd', probs_low, grad_full)
    return (query_grad, key_grad, value_grad)

def sequence_grads(operands, position):
    seq_queries, seq_keys, seq_values, seq_cots, seq_lse, seq_deltas = operands
    group_size = HQ // HK
    queries_head = jnp.moveaxis(seq_queries.reshape(SEQ, HK, group_size, DH), 1, 0)
    keys_head = jnp.moveaxis(seq_keys.reshape(SEQ, HK, DH), 1, 0)
    values_head = jnp.moveaxis(seq_values.reshape(SEQ, HK, DH), 1, 0)
    cots_head = jnp.moveaxis(seq_cots.reshape(SEQ, HK, group_size, DH), 1, 0)
    lse_head = seq_lse.reshape(HK, group_size, SEQ)
    deltas_head = seq_deltas.reshape(HK, group_size, SEQ)
    query_grad, key_grad, value_grad = lax.map(lambda group_ops: group_grads(group_ops, position), (queries_head, keys_head, values_head, cots_head, lse_head, deltas_head))
    query_grad = jnp.moveaxis(query_grad, 0, 1).reshape(SEQ, HQ * DH)
    key_grad = jnp.moveaxis(key_grad, 0, 1).reshape(SEQ, HK * DH)
    value_grad = jnp.moveaxis(value_grad, 0, 1).reshape(SEQ, HK * DH)
    return (query_grad.astype(jnp.bfloat16), key_grad.astype(jnp.bfloat16), value_grad.astype(jnp.bfloat16))

def reference(hidden_in, queries, key_states, value_states, grad_out, log_sums, deltas, block_order):
    row_ids = jnp.arange(SEQ, dtype=jnp.int32)
    position = (block_order[row_ids // BLOCK] * BLOCK + row_ids % BLOCK).astype(jnp.int32)
    grad_queries, grad_keys, grad_values = lax.map(lambda seq_ops: sequence_grads(seq_ops, position), (queries, key_states, value_states, grad_out, log_sums, deltas))
    flat_hidden = hidden_in.reshape(BATCH * SEQ, DIN)
    key_wgrad = jnp.dot(flat_hidden.T, grad_keys.reshape(BATCH * SEQ, HK * DH), preferred_element_type=jnp.float32)
    value_wgrad = jnp.dot(flat_hidden.T, grad_values.reshape(BATCH * SEQ, HK * DH), preferred_element_type=jnp.float32)
    return (grad_queries, grad_keys, grad_values, key_wgrad, value_wgrad)
```

```python
import functools
import math

import jax
import jax.numpy as jnp
from jax import lax
from jax.experimental import pallas as pl
from jax.experimental.pallas import tpu as pltpu
from jax.sharding import PartitionSpec as P

HQ = 16
HK = 4
DH = 128
GROUP = HQ // HK
MASKED = -1e30
MESH = pl.DeviceIdType.MESH
NT = (((1,), (1,)), ((), ()))
TN = (((0,), (0,)), ((), ()))
NN = (((1,), (0,)), ((), ()))


def dot(left, right, dims):
    return lax.dot_general(left, right, dims, preferred_element_type=jnp.float32)


def kernel(
    sizes,
    order_ref, hid_ref, q_ref, k_ref, v_ref, do_ref, lse_ref, delta_ref,
    dq_out, dk_out, dv_out, wk_out, wv_out,
    kv, qbuf, dobuf, lbuf, qst, dost, lst, qpos, dqt, dqs, acc, dsend, drecv,
    hall, gall, pf, pb, xrecv, zsend, zrecv, fin,
    kv_s, kv_r, q_s, q_r, l_sem, h_s, h_r, hf_s, hf_r, d_s, d_r, g_s, g_r,
    o_s, o_r, x_s, x_r, z_s, z_r,
):
    chips, nx, nz, rows, span = sizes
    b = lax.axis_index("batch")
    s = lax.axis_index("seq")
    c, p = s // 2, s % 2
    bz, bx = b // nx, b % nx
    qc = HQ * DH // 2
    kc = HK * DH // 2
    hh = HQ // 2
    hg = HK // 2

    def seq_peer(oc, q):
        return (b, ((c + oc) % chips) * 2 + (p + q) % 2)

    def fast_peer(ox):
        return (bz * nx + (bx + ox) % nx, s)

    def slow_peer(oz):
        return (((bz + oz) % nz) * nx + bx, s)

    def send(src, dst, ss, rs, peer):
        copy = pltpu.make_async_remote_copy(
            src_ref=src, dst_ref=dst, send_sem=ss, recv_sem=rs, device_id=peer, device_id_type=MESH
        )
        copy.start()
        return copy

    def cols(index, width):
        return pl.ds(pl.multiple_of(index * width, width), width)

    peers = [seq_peer(oc, q) for oc in range(chips) for q in range(2) if oc or q]
    peers += [fast_peer(ox) for ox in range(1, nx)] + [slow_peer(oz) for oz in range(1, nz)]
    barrier = pltpu.get_barrier_semaphore()
    for peer in peers:
        pl.semaphore_signal(barrier, inc=1, device_id=peer, device_id_type=MESH)
    pl.semaphore_wait(barrier, len(peers))

    sib = seq_peer(0, 1)
    mine, other = p, (p + 1) % 2
    kv_copies = {}
    for oc in list(range(1, chips)) + [0]:
        for q in range(2):
            if oc == 0 and q == 0:
                continue
            want = (p + q) % 2
            kv_copies[oc, q] = [
                send(ref.at[:, cols(want, kc)], kv.at[oc, q, i], kv_s.at[oc, q, i],
                     kv_r.at[oc, q, i], seq_peer(oc, q))
                for i, ref in enumerate((k_ref, v_ref))
            ]
    swaps = [
        send(q_ref.at[:, cols(other, qc)], qbuf, q_s.at[0], q_r.at[0], sib),
        send(do_ref.at[:, cols(other, qc)], dobuf, q_s.at[1], q_r.at[1], sib),
        send(lse_ref.at[cols(other, hh), :], lbuf.at[0], q_s.at[2], q_r.at[2], sib),
        send(delta_ref.at[cols(other, hh), :], lbuf.at[1], q_s.at[3], q_r.at[3], sib),
    ]
    own_hid = pltpu.make_async_copy(hid_ref.at[c], hall.at[0, 0], l_sem.at[0])
    own_hid.start()
    hid_copies = [
        send(hid_ref.at[(c + oc) % chips], hall.at[oc, 0], h_s.at[oc], h_r.at[oc], seq_peer(oc, 0))
        for oc in range(1, chips)
    ]
    hid_forward = [send(hid_ref.at[c], hall.at[0, 1], hf_s.at[0], hf_r.at[0], sib)]

    kv[0, 0, 0] = k_ref[:, cols(mine, kc)]
    kv[0, 0, 1] = v_ref[:, cols(mine, kc)]

    def block_pos(dev, shape, dim):
        row = lax.broadcasted_iota(jnp.int32, shape, dim)
        first = order_ref[dev * 2] * span
        second = order_ref[dev * 2 + 1] * span - span
        return row + jnp.where(row < span, first, second)

    half = GROUP * rows
    for q in range(2):
        if q:
            for copy in swaps:
                copy.wait()
        pos = block_pos(c * 2 + (p + q) % 2, (1, rows), 1)
        for g in range(hg):
            for h in range(GROUP):
                at = q * half + h * rows
                head = g * GROUP + h
                if q:
                    qst[g, at:at + rows, :] = qbuf[:, head * DH:(head + 1) * DH]
                    dost[g, at:at + rows, :] = dobuf[:, head * DH:(head + 1) * DH]
                    lst[g, 0, :, at:at + rows] = lbuf[0, head:head + 1, :]
                    lst[g, 1, :, at:at + rows] = lbuf[1, head:head + 1, :]
                else:
                    wide = cols(mine * hh + head, DH)
                    qst[g, at:at + rows, :] = q_ref[:, wide]
                    dost[g, at:at + rows, :] = do_ref[:, wide]
                    lst[g, 0, :, at:at + rows] = lse_ref[pl.ds(mine * hh + head, 1), :]
                    lst[g, 1, :, at:at + rows] = delta_ref[pl.ds(mine * hh + head, 1), :]
                if g == 0:
                    qpos[:, at:at + rows] = pos
    dqt[...] = jnp.zeros_like(dqt)
    scale = 1.0 / math.sqrt(DH)

    def key_block(oc, q, g):
        lane = cols(g, DH)
        keys, values = kv[oc, q, 0, :, lane], kv[oc, q, 1, :, lane]
        kpos = block_pos(((c + chips - oc) % chips) * 2 + (p + q) % 2, (rows, 1), 0)
        queries, cots = qst[g], dost[g]
        scores = jnp.where(kpos <= qpos[...], dot(keys, queries, NT) * scale, MASKED)
        probs = jnp.exp(scores - lst[g, 0])
        ds = (probs * (dot(values, cots, NT) - lst[g, 1]) * scale).astype(jnp.bfloat16)
        dv = dot(probs.astype(jnp.bfloat16), cots, NN)
        dk = dot(ds, queries, NN)
        dqt[g] += dot(keys, ds, TN)
        vlane = pl.ds(pl.multiple_of(kc + g * DH, DH), DH)
        if oc == 0:
            acc[q, :, lane] = dk
            acc[q, :, vlane] = dv
        else:
            dsend[oc, q, :, lane] = dk.astype(jnp.bfloat16)
            dsend[oc, q, :, vlane] = dv.astype(jnp.bfloat16)

    d_copies = {}
    for oc in range(chips):
        for q in range(2):
            for copy in kv_copies.get((oc, q), ()):
                copy.wait()

            @pl.loop(0, hg)
            def _(g, oc=oc, q=q):
                key_block(oc, q, g)

            if oc:
                d_copies[oc, q] = send(
                    dsend.at[oc, q], drecv.at[oc, q], d_s.at[oc, q], d_r.at[oc, q],
                    seq_peer(chips - oc, 0),
                )
    for oc in range(1, chips):
        hid_copies[oc - 1].wait()
        hid_forward.append(send(hall.at[oc, 0], hall.at[oc, 1], hf_s.at[oc], hf_r.at[oc], sib))

    for g in range(hg):
        turned = dqt[g].T.astype(jnp.bfloat16)
        for q in range(2):
            for h in range(GROUP):
                at = q * half + h * rows
                head = g * GROUP + h
                if q:
                    dqs[:, head * DH:(head + 1) * DH] = turned[at:at + rows]
                else:
                    dq_out[:, cols(mine * hh + head, DH)] = turned[at:at + rows]
    outs = [send(dqs, dq_out.at[:, cols(mine, qc)], o_s.at[0], o_r.at[0], sib)]

    g_copies = []
    for q in range(2):
        total = acc[q]
        for oc in range(1, chips):
            d_copies[oc, q].wait()
            total = total + drecv[oc, q].astype(jnp.float32)
        gall[0, q] = total.astype(jnp.bfloat16)
        for oc in range(1, chips):
            g_copies.append(
                send(gall.at[0, q], gall.at[oc, q], g_s.at[oc, q], g_r.at[oc, q], seq_peer(oc, 0))
            )
    dk_out[:, cols(mine, kc)] = gall[0, 0, :, :kc]
    dv_out[:, cols(mine, kc)] = gall[0, 0, :, kc:]
    outs += [
        send(gall.at[0, 1, :, :kc], dk_out.at[:, cols(mine, kc)], o_s.at[1], o_r.at[1], sib),
        send(gall.at[0, 1, :, kc:], dv_out.at[:, cols(mine, kc)], o_s.at[2], o_r.at[2], sib),
    ]

    own_hid.wait()
    for copy in hid_forward + g_copies:
        copy.wait()
    tokens = chips * 2 * rows
    hidden = hall[...].reshape(tokens, hall.shape[3])
    grads = gall[...].reshape(tokens, gall.shape[3])
    pf[...] = dot(hidden, grads, TN).reshape(pf.shape)
    pb[...] = pf[...].astype(jnp.bfloat16)
    x_copies = {}
    for oz in list(range(1, nz)) + [0]:
        for ox in range(1, nx):
            x_copies[ox, oz] = send(
                pb.at[(bx + ox) % nx, (bz + oz) % nz], xrecv.at[ox, oz], x_s.at[ox, oz],
                x_r.at[ox, oz], fast_peer(ox),
            )
    z_copies = []
    for oz in list(range(1, nz)) + [0]:
        total = pf[bx, (bz + oz) % nz]
        for ox in range(1, nx):
            x_copies[ox, oz].wait()
            total = total + xrecv[ox, oz].astype(jnp.float32)
        if oz:
            zsend[oz] = total.astype(jnp.bfloat16)
            z_copies.append(
                send(zsend.at[oz], zrecv.at[oz], z_s.at[oz], z_r.at[oz], slow_peer(oz))
            )
    for oz in range(1, nz):
        z_copies[oz - 1].wait()
        total = total + zrecv[oz].astype(jnp.float32)
    fin[...] = total.reshape(fin.shape)
    outs += [
        send(fin.at[other, :, :kc], wk_out.at[:, cols(mine, kc)], o_s.at[3], o_r.at[3], sib),
        send(fin.at[other, :, kc:], wv_out.at[:, cols(mine, kc)], o_s.at[4], o_r.at[4], sib),
    ]
    wk_out[:, cols(mine, kc)] = fin[mine, :, :kc]
    wv_out[:, cols(mine, kc)] = fin[mine, :, kc:]
    for copy in outs:
        copy.wait()


def solution(mesh):
    batch, seq = mesh.shape["batch"], mesh.shape["seq"]
    chips = seq // 2
    nx = 2 if batch <= 8 else batch // 2
    nz = batch // nx

    def shards(hidden, queries, keys, values, cots, lse, deltas, order):
        rows, din = hidden.shape[1], hidden.shape[2]
        qw, kw = queries.shape[2], keys.shape[2]
        part = din // chips
        two = part // batch
        hid = hidden.reshape(rows, nz, nx, chips, two).transpose(3, 0, 2, 1, 4)
        hid = hid.reshape(chips, rows, part)
        bf, f32 = jnp.bfloat16, jnp.float32
        hg = HK // 2
        wide = 2 * GROUP * rows
        vmem = pl.BlockSpec(memory_space=pltpu.VMEM)
        dma = pltpu.SemaphoreType.DMA
        V = pltpu.VMEM
        outs = pl.pallas_call(
            functools.partial(kernel, (chips, nx, nz, rows, rows // 2)),
            out_shape=[
                jax.ShapeDtypeStruct((rows, qw), bf),
                jax.ShapeDtypeStruct((rows, kw), bf),
                jax.ShapeDtypeStruct((rows, kw), bf),
                jax.ShapeDtypeStruct((two // 2, kw), f32),
                jax.ShapeDtypeStruct((two // 2, kw), f32),
            ],
            in_specs=[pl.BlockSpec(memory_space=pltpu.SMEM)] + [vmem] * 7,
            out_specs=[vmem] * 5,
            scratch_shapes=[
                V((chips, 2, 2, rows, kw // 2), bf),
                V((rows, qw // 2), bf),
                V((rows, qw // 2), bf),
                V((2, HQ // 2, rows), f32),
                V((hg, wide, DH), bf),
                V((hg, wide, DH), bf),
                V((hg, 2, 1, wide), f32),
                V((1, wide), jnp.int32),
                V((hg, DH, wide), f32),
                V((rows, qw // 2), bf),
                V((2, rows, kw), f32),
                V((chips, 2, rows, kw), bf),
                V((chips, 2, rows, kw), bf),
                V((chips, 2, rows, part), bf),
                V((chips, 2, rows, kw), bf),
                V((nx, nz, two, kw), f32),
                V((nx, nz, two, kw), bf),
                V((nx, nz, two, kw), bf),
                V((nz, two, kw), bf),
                V((nz, two, kw), bf),
                V((2, two // 2, kw), f32),
                dma((chips, 2, 2)), dma((chips, 2, 2)),
                dma((4,)), dma((4,)), dma((1,)),
                dma((chips,)), dma((chips,)), dma((chips,)), dma((chips,)),
                dma((chips, 2)), dma((chips, 2)), dma((chips, 2)), dma((chips, 2)),
                dma((5,)), dma((5,)),
                dma((nx, nz)), dma((nx, nz)), dma((nz,)), dma((nz,)),
            ],
            compiler_params=pltpu.CompilerParams(
                collective_id=0, has_side_effects=True, vmem_limit_bytes=56 * 1024 * 1024
            ),
        )(order, hid, queries[0], keys[0], values[0], cots[0], lse[0], deltas[0])
        dq, dk, dv, wk, wv = outs
        return dq[None], dk[None], dv[None], wk, wv

    rows_spec = P("batch", "seq", None)
    in_specs = (rows_spec,) * 5 + (P("batch", None, "seq"),) * 2 + (P(),)
    weight_spec = P(("batch", "seq"), None)
    out_specs = (rows_spec,) * 3 + (weight_spec,) * 2
    return jax.shard_map(shards, mesh=mesh, in_specs=in_specs, out_specs=out_specs, check_vma=False)
```

```python
import functools
import math

import jax
import jax.numpy as jnp
from jax import lax
from jax.experimental import pallas as pl
from jax.experimental.pallas import tpu as pltpu
from jax.sharding import PartitionSpec as P

HQ = 16
HK = 4
DH = 128
GROUP = HQ // HK
MASKED = -1e30
MESH = pl.DeviceIdType.MESH
NT = (((1,), (1,)), ((), ()))
TN = (((0,), (0,)), ((), ()))
NN = (((1,), (0,)), ((), ()))


def dot(left, right, dims):
    return lax.dot_general(left, right, dims, preferred_element_type=jnp.float32)


def kernel(
    sizes,
    order_ref, hid_ref, q_ref, k_ref, v_ref, do_ref, lse_ref, delta_ref,
    dq_out, dk_out, dv_out, wk_out, wv_out,
    kv, qbuf, dobuf, lbuf, qst, dost, lst, qpos, dqt, dqs, acc, dsend, drecv,
    hall, gall, pf, pb, xrecv, zsend, zrecv, fin,
    kv_s, kv_r, q_s, q_r, l_sem, h_s, h_r, hf_s, hf_r, d_s, d_r, g_s, g_r,
    o_s, o_r, w_s, w_r, x_s, x_r, z_s, z_r,
):
    chips, nx, nz, rows, span, two, strips = sizes
    b = lax.axis_index("batch")
    s = lax.axis_index("seq")
    c, p = s // 2, s % 2
    bz, bx = b // nx, b % nx
    qc = HQ * DH // 2
    kc = HK * DH // 2
    hh = HQ // 2
    hg = HK // 2

    def seq_peer(oc, q):
        return (b, ((c + oc) % chips) * 2 + (p + q) % 2)

    def fast_peer(ox):
        return (bz * nx + (bx + ox) % nx, s)

    def slow_peer(oz):
        return (((bz + oz) % nz) * nx + bx, s)

    def remote(src, dst, ss, rs, peer):
        return pltpu.make_async_remote_copy(
            src_ref=src, dst_ref=dst, send_sem=ss, recv_sem=rs, device_id=peer, device_id_type=MESH
        )

    def send(src, dst, ss, rs, peer):
        copy = remote(src, dst, ss, rs, peer)
        copy.start()
        return copy

    def cols(index, width):
        return pl.ds(pl.multiple_of(index * width, width), width)

    def slot(oc, q):
        return pl.ds((oc * 2 + q) * rows, rows)

    peers = [seq_peer(oc, q) for oc in range(chips) for q in range(2) if oc or q]
    peers += [fast_peer(ox) for ox in range(1, nx)] + [slow_peer(oz) for oz in range(1, nz)]
    barrier = pltpu.get_barrier_semaphore()
    for peer in peers:
        pl.semaphore_signal(barrier, inc=1, device_id=peer, device_id_type=MESH)
    pl.semaphore_wait(barrier, len(peers))

    sib = seq_peer(0, 1)
    mine, other = p, (p + 1) % 2
    kv_copies = {}
    for oc in list(range(1, chips)) + [0]:
        for g in range(hg):
            for q in range(2):
                if oc == 0 and q == 0:
                    continue
                want = (p + q) % 2
                kv_copies[oc, g, q] = [
                    send(ref.at[:, cols(want * hg + g, DH)], kv.at[oc, g, q, i],
                         kv_s.at[oc, g, q, i], kv_r.at[oc, g, q, i], seq_peer(oc, q))
                    for i, ref in enumerate((k_ref, v_ref))
                ]
    swaps = [
        send(q_ref.at[:, cols(other, qc)], qbuf, q_s.at[0], q_r.at[0], sib),
        send(do_ref.at[:, cols(other, qc)], dobuf, q_s.at[1], q_r.at[1], sib),
        send(lse_ref.at[cols(other, hh), :], lbuf.at[0], q_s.at[2], q_r.at[2], sib),
        send(delta_ref.at[cols(other, hh), :], lbuf.at[1], q_s.at[3], q_r.at[3], sib),
    ]

    def pieces(oc, ox, q):
        to_chip, to_fast = (c + oc) % chips, (bx + ox) % nx
        if not strips:
            return [(hid_ref.at[to_chip, to_fast], hall.at[ox, slot(oc, q), :])]
        return [
            (hid_ref.at[:, cols((z * nx + to_fast) * chips + to_chip, two)],
             hall.at[ox, slot(oc, q), z * two:(z + 1) * two])
            for z in range(nz)
        ]

    def hid_send(oc, ox, q, ss, rs, peer):
        for src, dst in pieces(oc, ox, q):
            remote(src, dst, ss, rs, peer).start()
        whole = hall.at[ox, slot(oc, q), :]
        return remote(whole, whole, ss, rs, peer)

    fast_order = list(range(1, nx)) + [0]
    hid_copies = {}
    hid_forward = {}

    def hid_part(ox):
        for oc in range(1, chips):
            hid_copies[oc, ox] = hid_send(
                oc, ox, 0, h_s.at[oc, ox], h_r.at[oc, ox], seq_peer(oc, 0)
            )

    for ox in fast_order[:-1]:
        hid_part(ox)
    hid_local = {}
    for ox in fast_order:
        hid_forward[0, ox] = hid_send(0, ox, 1, hf_s.at[0, ox], hf_r.at[0, ox], sib)
        for src, dst in pieces(0, ox, 0):
            pltpu.make_async_copy(src, dst, l_sem.at[ox]).start()
        whole = hall.at[ox, slot(0, 0), :]
        hid_local[ox] = pltpu.make_async_copy(whole, whole, l_sem.at[ox])

    for g in range(hg):
        lane = cols(mine * hg + g, DH)
        kv[0, g, 0, 0] = k_ref[:, lane]
        kv[0, g, 0, 1] = v_ref[:, lane]

    def block_pos(dev, shape, dim):
        row = lax.broadcasted_iota(jnp.int32, shape, dim)
        first = order_ref[dev * 2] * span
        second = order_ref[dev * 2 + 1] * span - span
        return row + jnp.where(row < span, first, second)

    half = GROUP * rows
    for q in range(2):
        if q:
            for copy in swaps:
                copy.wait()
        pos = block_pos(c * 2 + (p + q) % 2, (1, rows), 1)
        for g in range(hg):
            for h in range(GROUP):
                at = q * half + h * rows
                head = g * GROUP + h
                if q:
                    qst[g, at:at + rows, :] = qbuf[:, head * DH:(head + 1) * DH]
                    dost[g, at:at + rows, :] = dobuf[:, head * DH:(head + 1) * DH]
                    lst[g, 0, :, at:at + rows] = lbuf[0, head:head + 1, :]
                    lst[g, 1, :, at:at + rows] = lbuf[1, head:head + 1, :]
                else:
                    wide = cols(mine * hh + head, DH)
                    qst[g, at:at + rows, :] = q_ref[:, wide]
                    dost[g, at:at + rows, :] = do_ref[:, wide]
                    lst[g, 0, :, at:at + rows] = lse_ref[pl.ds(mine * hh + head, 1), :]
                    lst[g, 1, :, at:at + rows] = delta_ref[pl.ds(mine * hh + head, 1), :]
                if g == 0:
                    qpos[:, at:at + rows] = pos
    dqt[...] = jnp.zeros_like(dqt)
    scale = 1.0 / math.sqrt(DH)

    def key_block(oc, q, g):
        keys, values = kv[oc, g, q, 0], kv[oc, g, q, 1]
        kpos = block_pos(((c + chips - oc) % chips) * 2 + (p + q) % 2, (rows, 1), 0)
        queries, cots = qst[g], dost[g]
        scores = jnp.where(kpos <= qpos[...], dot(keys, queries, NT) * scale, MASKED)
        probs = jnp.exp(scores - lst[g, 0])
        ds = (probs * (dot(values, cots, NT) - lst[g, 1]) * scale).astype(jnp.bfloat16)
        dv = dot(probs.astype(jnp.bfloat16), cots, NN)
        dk = dot(ds, queries, NN)
        dqt[g] += dot(keys, ds, TN)
        if oc == 0:
            acc[g, q, :, :DH] = dk
            acc[g, q, :, DH:] = dv
        else:
            dsend[oc, g, q, :, :DH] = dk.astype(jnp.bfloat16)
            dsend[oc, g, q, :, DH:] = dv.astype(jnp.bfloat16)

    d_copies = {}
    for oc in range(chips):
        for g in range(hg):
            for q in range(2):
                for copy in kv_copies.get((oc, g, q), ()):
                    copy.wait()

            @pl.loop(0, 2)
            def _(q, oc=oc, g=g):
                key_block(oc, q, g)

            if oc:
                d_copies[oc, g] = send(
                    dsend.at[oc, g], drecv.at[oc, g], d_s.at[oc, g], d_r.at[oc, g],
                    seq_peer(chips - oc, 0),
                )

    def hid_on(ox):
        for oc in range(1, chips):
            hid_copies[oc, ox].wait()
            whole = hall.at[ox, slot(oc, 1), :]
            hid_forward[oc, ox] = send(
                hall.at[ox, slot(oc, 0), :], whole, hf_s.at[oc, ox], hf_r.at[oc, ox], sib
            )

    for ox in fast_order[:-1]:
        hid_on(ox)

    for g in range(hg):
        turned = dqt[g].T.astype(jnp.bfloat16)
        for q in range(2):
            for h in range(GROUP):
                at = q * half + h * rows
                head = g * GROUP + h
                if q:
                    dqs[:, head * DH:(head + 1) * DH] = turned[at:at + rows]
                else:
                    dq_out[:, cols(mine * hh + head, DH)] = turned[at:at + rows]
    outs = [send(dqs, dq_out.at[:, cols(mine, qc)], o_s.at[0], o_r.at[0], sib)]

    g_copies = {}
    both = pl.ds(0, 2 * rows)
    for g in range(hg):
        total = acc[g]
        for oc in range(1, chips):
            d_copies[oc, g].wait()
            total = total + drecv[oc, g].astype(jnp.float32)
        gall[g, both, :] = total.astype(jnp.bfloat16).reshape(2 * rows, 2 * DH)
        for oc in range(1, chips):
            g_copies[oc, g] = send(
                gall.at[g, both, :], gall.at[g, pl.ds(oc * 2 * rows, 2 * rows), :],
                g_s.at[oc, g], g_r.at[oc, g], seq_peer(oc, 0),
            )
        if g == 0:
            hid_part(0)
    for g in range(hg):
        lane = cols(mine * hg + g, DH)
        for i, out in enumerate((dk_out, dv_out)):
            piece = slice(i * DH, (i + 1) * DH)
            out[:, lane] = gall[g, :rows, piece]
            outs.append(
                send(gall.at[g, rows:2 * rows, piece], out.at[:, lane],
                     o_s.at[1 + 2 * g + i], o_r.at[1 + 2 * g + i], sib)
            )

    def ready(ox):
        hid_local[ox].wait()
        for oc in range(chips):
            hid_forward[oc, ox].wait()

    def product(ox, g):
        return dot(hall[ox], gall[g], TN).reshape(nz, two, 2 * DH)

    slow_order = list(range(1, nz)) + [0]
    x_copies = {}
    for ox in fast_order[:-1]:
        ready(ox)
    for g in range(hg):
        for oc in range(1, chips):
            g_copies[oc, g].wait()
        for ox in fast_order[:-1]:
            pb[g, ox] = product(ox, g).astype(jnp.bfloat16)
        for oz in slow_order:
            for ox in fast_order[:-1]:
                x_copies[g, ox, oz] = send(
                    pb.at[g, ox, (bz + oz) % nz], xrecv.at[g, ox, oz], x_s.at[g, ox, oz],
                    x_r.at[g, ox, oz], fast_peer(ox),
                )
        if g == 0:
            hid_on(0)
            ready(0)
        pf[g] = product(0, g)

    def gathered(g, oz):
        total = pf[g, (bz + oz) % nz]
        for ox in fast_order[:-1]:
            x_copies[g, ox, oz].wait()
            total = total + xrecv[g, ox, oz].astype(jnp.float32)
        return total

    z_copies = {}
    for g in range(hg):
        for oz in slow_order[:-1]:
            zsend[g, oz] = gathered(g, oz).astype(jnp.bfloat16)
            z_copies[g, oz] = send(
                zsend.at[g, oz], zrecv.at[g, oz], z_s.at[g, oz], z_r.at[g, oz], slow_peer(oz)
            )
    for g in range(hg):
        total = gathered(g, 0)
        for oz in slow_order[:-1]:
            z_copies[g, oz].wait()
            total = total + zrecv[g, oz].astype(jnp.float32)
        fin[g] = total.reshape(2, two // 2, 2 * DH)
        lane = cols(mine * hg + g, DH)
        for i, out in enumerate((wk_out, wv_out)):
            piece = slice(i * DH, (i + 1) * DH)
            outs.append(
                send(fin.at[g, other, :, piece], out.at[:, lane], w_s.at[g, i], w_r.at[g, i], sib)
            )
            out[:, lane] = fin[g, mine, :, piece]
    for copy in outs:
        copy.wait()


def solution(mesh):
    batch, seq = mesh.shape["batch"], mesh.shape["seq"]
    chips = seq // 2
    nx = 2 if batch <= 8 else batch // 2
    nz = batch // nx

    def shards(hidden, queries, keys, values, cots, lse, deltas, order):
        rows, din = hidden.shape[1], hidden.shape[2]
        qw, kw = queries.shape[2], keys.shape[2]
        part = din // chips
        two = part // batch
        strips = two % 128 == 0
        if strips:
            hid = hidden[0]
        else:
            hid = hidden.reshape(rows, nz, nx, chips, two).transpose(3, 2, 0, 1, 4)
            hid = hid.reshape(chips, nx, rows, nz * two)
        bf, f32 = jnp.bfloat16, jnp.float32
        hg = HK // 2
        wide = 2 * GROUP * rows
        vmem = pl.BlockSpec(memory_space=pltpu.VMEM)
        dma = pltpu.SemaphoreType.DMA
        V = pltpu.VMEM
        outs = pl.pallas_call(
            functools.partial(kernel, (chips, nx, nz, rows, rows // 2, two, strips)),
            out_shape=[
                jax.ShapeDtypeStruct((rows, qw), bf),
                jax.ShapeDtypeStruct((rows, kw), bf),
                jax.ShapeDtypeStruct((rows, kw), bf),
                jax.ShapeDtypeStruct((two // 2, kw), f32),
                jax.ShapeDtypeStruct((two // 2, kw), f32),
            ],
            in_specs=[pl.BlockSpec(memory_space=pltpu.SMEM)] + [vmem] * 7,
            out_specs=[vmem] * 5,
            scratch_shapes=[
                V((chips, hg, 2, 2, rows, DH), bf),
                V((rows, qw // 2), bf),
                V((rows, qw // 2), bf),
                V((2, HQ // 2, rows), f32),
                V((hg, wide, DH), bf),
                V((hg, wide, DH), bf),
                V((hg, 2, 1, wide), f32),
                V((1, wide), jnp.int32),
                V((hg, DH, wide), f32),
                V((rows, qw // 2), bf),
                V((hg, 2, rows, 2 * DH), f32),
                V((chips, hg, 2, rows, 2 * DH), bf),
                V((chips, hg, 2, rows, 2 * DH), bf),
                V((nx, chips * 2 * rows, nz * two), bf),
                V((hg, chips * 2 * rows, 2 * DH), bf),
                V((hg, nz, two, 2 * DH), f32),
                V((hg, nx, nz, two, 2 * DH), bf),
                V((hg, nx, nz, two, 2 * DH), bf),
                V((hg, nz, two, 2 * DH), bf),
                V((hg, nz, two, 2 * DH), bf),
                V((hg, 2, two // 2, 2 * DH), f32),
                dma((chips, hg, 2, 2)), dma((chips, hg, 2, 2)),
                dma((4,)), dma((4,)), dma((nx,)),
                dma((chips, nx)), dma((chips, nx)), dma((chips, nx)), dma((chips, nx)),
                dma((chips, hg)), dma((chips, hg)), dma((chips, hg)), dma((chips, hg)),
                dma((1 + 2 * hg,)), dma((1 + 2 * hg,)), dma((hg, 2)), dma((hg, 2)),
                dma((hg, nx, nz)), dma((hg, nx, nz)), dma((hg, nz)), dma((hg, nz)),
            ],
            compiler_params=pltpu.CompilerParams(
                collective_id=0, has_side_effects=True, vmem_limit_bytes=56 * 1024 * 1024
            ),
        )(order, hid, queries[0], keys[0], values[0], cots[0], lse[0], deltas[0])
        dq, dk, dv, wk, wv = outs
        return dq[None], dk[None], dv[None], wk, wv

    rows_spec = P("batch", "seq", None)
    in_specs = (rows_spec,) * 5 + (P("batch", None, "seq"),) * 2 + (P(),)
    weight_spec = P(("batch", "seq"), None)
    out_specs = (rows_spec,) * 3 + (weight_spec,) * 2
    return jax.shard_map(shards, mesh=mesh, in_specs=in_specs, out_specs=out_specs, check_vma=False)
```
